256 devices in a mesh: ent: 8 (over x, core), blk: 4 (over y), rel: 8 (over z).
Axes of the slice: x: 4, y: 4, z: 8, core: 2. Of those that a mesh axis runs over, the one named last changes fastest.
Arguments:
- factors: bfloat16 [32768, 256], P(('ent', 'blk')), may hold values from -12 to 12
- heads: int32 [32, 8, 1, 32768], P(None, 'rel', None, ('ent', 'blk')), may hold values from 0 to 1023, as said below
- tails: int32 [32, 8, 1, 32768], P(None, 'rel', None, ('ent', 'blk')), may hold values from 0 to 1023, as said below
- values: float32 [32, 8, 1, 32768], P(None, 'rel', None, ('ent', 'blk')), may hold values from 0.3 to 9
Outputs:
- relation_fit: float32 [256, 256, 256], P(('ent', 'blk', 'rel'))
- residual: float32 [256, 256, 256], P(('ent', 'blk', 'rel'))
The draws below stay inside these ranges and needn't reach their ends.
Inputs may be any that keep to these rules, and one draw needn't show every extreme that they name: In every aligned tile of 128 triple columns (columns 128 t to 128 t + 127 of one relation) all heads lie in one aligned block of 128 positions (128 b to 128 b + 127). In every aligned tile of 128 triple columns all tails lie in one aligned block of 128 positions.
All inputs are finite; a program needn't handle non-finite values.
Results may differ from the reference program's by a relative error of at most 0.0029.
Values sent between devices are 32-bit elements; how exact they have to be, the bound alone decides.
No kernel may reach another device: no remote copies, remote signals or barrier semaphores. Data moves between devices by JAX's collectives and lax.ppermute only.
A program may use at most 128 MiB of HBM per device.

```python
import math
import jax
import jax.numpy as jnp
from jax import lax

RANK = 256
ENT_DEV = 1024
TRIP = 1024
REL_DEV = 1
ITERS = 8
SHARDS = 32
ENTS = 32768
RELS = 256
N_REL = 8


def draw_factors(key, part):
    keys = jax.random.split(jax.random.fold_in(key, 11), 3)
    entries = jnp.clip(jax.random.normal(keys[0], (ENTS, RANK), jnp.float32), -6.0, 6.0)
    columns = jnp.exp(jax.random.uniform(keys[1], (RANK,), jnp.float32, math.log(0.1), 0.0))
    row_scale = jnp.exp(jax.random.uniform(keys[2], (ENTS, 1), jnp.float32, math.log(0.5), math.log(2.0)))
    return (entries * columns[None, :] * row_scale).astype(jnp.bfloat16)


def tiled_positions(key, salt):
    keys = jax.random.split(jax.random.fold_in(key, salt), 2)
    tile_count = SHARDS * TRIP // 128
    block_ids = jax.random.randint(keys[0], (SHARDS, N_REL, REL_DEV, tile_count, 1), 0, ENT_DEV // 128, jnp.int32)
    inside = jax.random.randint(keys[1], (SHARDS, N_REL, REL_DEV, tile_count, 128), 0, 128, jnp.int32)
    return (block_ids * 128 + inside).reshape(SHARDS, N_REL, REL_DEV, SHARDS * TRIP).astype(jnp.int32)


def draw_heads(key, part):
    return tiled_positions(key, 31)


def draw_tails(key, part):
    return tiled_positions(key, 47)


def draw_values(key, part):
    shape_all = (SHARDS, N_REL, REL_DEV, SHARDS * TRIP)
    sub_key = jax.random.fold_in(key, 23)
    base_values = jnp.exp(jax.random.uniform(sub_key, shape_all, jnp.float32, math.log(0.5), math.log(2.0)))
    first_index = jnp.arange(SHARDS, dtype=jnp.int32)[:, None, None, None]
    second_index = jnp.arange(N_REL, dtype=jnp.int32)[None, :, None, None]
    third_index = jnp.arange(REL_DEV, dtype=jnp.int32)[None, None, :, None]
    relation_index = ((first_index * N_REL + second_index) * REL_DEV + third_index).astype(jnp.float32)
    rising = 1.0 + 2.0 * relation_index / max(RELS - 1, 1)
    return (base_values * rising).astype(jnp.float32)


def setup_inputs(seed: int = 0) -> dict:
    streams_of = jax.random.split(jax.random.key(seed), 5)
    factors = draw_factors(jax.random.fold_in(streams_of[4], 71), 0)
    heads = draw_heads(jax.random.fold_in(streams_of[4], 71), 0)
    tails = draw_tails(jax.random.fold_in(streams_of[4], 71), 0)
    values = draw_values(jax.random.fold_in(streams_of[4], 71), 0)
    return dict(factors=factors, heads=heads, tails=tails, values=values)


ridge_weight = 0.01

def apply_normal(gram_matrix, stacked):
    left_side = jnp.einsum('ab,kbc->kac', gram_matrix, stacked, precision=lax.Precision.HIGHEST)
    return jnp.einsum('kac,cd->kad', left_side, gram_matrix, precision=lax.Precision.HIGHEST) + ridge_weight * stacked

def reference(factors, heads, tails, values):
    gram_matrix = jnp.dot(factors.T, factors, preferred_element_type=jnp.float32) / ENTS
    column_ids = jnp.arange(SHARDS * TRIP, dtype=jnp.int32)
    offsets = (column_ids // TRIP * ENT_DEV).astype(jnp.int32)
    head_ids = (heads.reshape(RELS, SHARDS * TRIP) + offsets).astype(jnp.int32)
    tail_ids = (tails.reshape(RELS, SHARDS * TRIP) + offsets).astype(jnp.int32)
    weights = values.reshape(RELS, SHARDS * TRIP)
    norm_scale = 1.0 / math.sqrt(SHARDS * TRIP)

    def single(operands):
        head_row, tail_row, weight_row = operands
        weighted = (weight_row[:, None] * jnp.take(factors, head_row, axis=0).astype(jnp.float32)).astype(jnp.bfloat16)
        tail_rows = jnp.take(factors, tail_row, axis=0)
        return jnp.dot(weighted.T, tail_rows, preferred_element_type=jnp.float32) * norm_scale
    target = lax.map(single, (head_ids, tail_ids, weights))
    fitted = jnp.zeros_like(target)
    residual = target
    direction = target
    norm_now = jnp.sum(residual * residual)
    for step_index in range(ITERS):
        image_map = apply_normal(gram_matrix, direction)
        step_size = norm_now / jnp.sum(direction * image_map)
        fitted = fitted + step_size * direction
        residual = residual - step_size * image_map
        norm_next = jnp.sum(residual * residual)
        direction = residual + norm_next / norm_now * direction
        norm_now = norm_next
    return (fitted, residual)
```

```python
import functools
import math

import jax
import jax.numpy as jnp
from jax import lax
from jax.experimental import pallas as pl
from jax.experimental.pallas import tpu as pltpu
from jax.sharding import Mesh
from jax.sharding import PartitionSpec as P

F32 = jnp.float32
BF16 = jnp.bfloat16
ITERS = 8
TILE = 128
RIDGE = 0.01
TINY = 1e-12
ENT_BLK_REL = ("ent_0", "ent_1", "blk", "rel")
ENT_BLK = ("ent_0", "ent_1", "blk")
BASIS = ITERS + 1
PAIRS = [(i, j) for j in range(BASIS) for i in range(j + 1)]
PAIR_ROWS = -(-len(PAIRS) // 8) * 8


def tables_kernel(factors_ref, table_ref, gram_ref):
    gram = None
    for b in range(factors_ref.shape[0] // TILE):
        rows = factors_ref[b * TILE : (b + 1) * TILE, :]
        columns = rows.astype(F32).T
        table_ref[b] = columns
        part = jnp.dot(columns.astype(BF16), rows, preferred_element_type=F32)
        gram = part if gram is None else gram + part
    gram_ref[...] = gram


def resident(*arrays):
    return tuple(pltpu.with_memory_space_constraint(a, pltpu.VMEM) for a in arrays)


LEAN = pltpu.CompilerParams(vmem_limit_bytes=16 * 2**20)
IN_VMEM = pl.BlockSpec(memory_space=pltpu.VMEM)
IN_SMEM = pl.BlockSpec(memory_space=pltpu.SMEM)


def tables(factors):
    ents, rank = factors.shape
    return pl.pallas_call(
        tables_kernel,
        out_shape=(
            pltpu.VMEM((ents // TILE, rank, TILE), F32),
            jax.ShapeDtypeStruct((rank, rank), F32),
        ),
        compiler_params=LEAN,
        name="tables",
    )(factors)


def lane_pick(block, ids):
    dims = lax.GatherDimensionNumbers(
        offset_dims=(),
        collapsed_slice_dims=(1,),
        start_index_map=(1,),
        operand_batching_dims=(0,),
        start_indices_batching_dims=(0,),
    )
    return lax.gather(
        block, ids[..., None], dims, (1, 1), mode=lax.GatherScatterMode.PROMISE_IN_BOUNDS
    )


def triple_kernel(order_ref, heads_ref, tails_ref, values_ref, table_ref, *rest, which, scale, halves):
    if halves:
        partner_ref, upper_ref, lower_ref, w_ref, t_ref = rest
    else:
        out_ref, w_ref, t_ref = rest
    rank = table_ref.shape[1]

    def rows(ids_ref, relation, tile):
        at = slice(tile * TILE, (tile + 1) * TILE)
        block = ids_ref[relation, 0, tile * TILE] // TILE
        inside = jnp.broadcast_to(ids_ref[relation, :, at] & (TILE - 1), (rank, TILE))
        return lane_pick(table_ref[block], inside).astype(BF16)

    for i in range(order_ref.shape[1]):
        relation = order_ref[which, i]
        slot = i % 2
        for tile in range(heads_ref.shape[2] // TILE):
            at = slice(tile * TILE, (tile + 1) * TILE)
            head_rows = rows(heads_ref, relation, tile).astype(F32)
            w_ref[slot, :, at] = (head_rows * values_ref[relation, :, at]).astype(BF16)
            t_ref[slot, :, at] = rows(tails_ref, relation, tile)
        summed = lax.dot_general(
            w_ref[slot], t_ref[slot], (((1,), (1,)), ((), ())), preferred_element_type=F32
        )
        summed = summed * scale
        if halves:
            summed = summed + partner_ref[i]
            upper_ref[i] = summed[: rank // 2]
            lower_ref[i] = summed[rank // 2 :]
        else:
            out_ref[i] = summed


def triple_sums(which, order, heads, tails, values, table, scale, partner=None):
    count = order.shape[1]
    width = heads.shape[2]
    rank = table.shape[1]
    args = [order, heads, tails, values, table]
    if partner is None:
        shape = pltpu.VMEM((count, rank, rank), F32)
    else:
        args.extend(resident(partner))
        shape = (pltpu.VMEM((count, rank // 2, rank), F32),) * 2
    return pl.pallas_call(
        functools.partial(triple_kernel, which=which, scale=scale, halves=partner is not None),
        in_specs=[IN_SMEM] + [IN_VMEM] * (len(args) - 1),
        out_shape=shape,
        scratch_shapes=[pltpu.VMEM((2, rank, width), BF16)] * 2,
        compiler_params=LEAN,
        name="triples_own" if partner is not None else "triples_partner",
    )(*args)


def total(array):
    return jnp.sum(jnp.sum(array, axis=0, keepdims=True), axis=1, keepdims=True)


def split(array):
    high = array.astype(BF16)
    return high, (array - high.astype(F32)).astype(BF16)


def dot(a, b):
    return jnp.dot(a, b, preferred_element_type=F32)


def signs(rank):
    i = lax.broadcasted_iota(jnp.int32, (rank, rank), 0)
    j = lax.broadcasted_iota(jnp.int32, (rank, rank), 1)
    mixed = i * 40503 + j * 30011 + 12345
    for step in (7, 3):
        mixed = mixed ^ lax.shift_right_logical(mixed, jnp.full_like(mixed, step * 2))
        mixed = mixed * 739982445
    mixed = mixed ^ lax.shift_right_logical(mixed, jnp.full_like(mixed, 15))
    return jnp.where((mixed & 64) == 0, 1.0, -1.0).astype(F32)


def recurrence_kernel(gram_ref, coef_ref):
    gram = gram_ref[...]
    rank = gram.shape[0]
    norm2 = total(gram * gram)
    inverse = lax.rsqrt(norm2)
    scaled = (gram * inverse).astype(BF16)

    def image(v):
        return dot(scaled, dot(v.astype(BF16), scaled).astype(BF16))

    def put(row, value):
        coef_ref[row : row + 1, :] = jnp.broadcast_to(value, (1, rank))

    put(0, inverse)
    put(1, norm2)
    now = signs(rank)
    ahead = image(now)
    size = lax.rsqrt(jnp.maximum(total(now * ahead), TINY))
    now = now * size
    ahead = ahead * size
    before = None
    off = None
    for step in range(ITERS):
        diagonal = total(ahead * ahead)
        rest = ahead - diagonal * now
        if before is not None:
            rest = rest - off * before
        rest_image = image(rest)
        square = jnp.maximum(total(rest * rest_image), TINY)
        inverse_off = lax.rsqrt(square)
        off = square * inverse_off
        put(2 + step, diagonal)
        put(2 + ITERS + step, off)
        put(2 + 2 * ITERS + step, inverse_off)
        before = now
        now = rest * inverse_off
        ahead = rest_image * inverse_off


COEF_ROWS = -(-(2 + 3 * ITERS) // 8) * 8


def recurrence(gram):
    return pl.pallas_call(
        recurrence_kernel,
        out_shape=pltpu.VMEM((COEF_ROWS, gram.shape[0]), F32),
        in_specs=[IN_VMEM],
        compiler_params=LEAN,
        name="recurrence",
    )(*resident(gram))


def basis_kernel(gram_ref, coef_ref, ua_ref, ub_ref, la_ref, lb_ref, basis_ref, inner_ref, sums_ref):
    rank = gram_ref.shape[0]
    half = rank // 2
    scaled = gram_ref[...] * coef_ref[0:1, :]
    g_high, g_low = split(scaled)
    basis_ref[0, :half, :] = ua_ref[...] + ub_ref[...]
    basis_ref[0, half:, :] = la_ref[...] + lb_ref[...]
    sums_ref[...] = jnp.zeros_like(sums_ref)
    row = 0
    for step in range(BASIS):
        now = basis_ref[step]
        if step < ITERS:
            v_high, v_low = split(now)
            right = dot(v_high, g_high) + (dot(v_low, g_high) + dot(v_high, g_low))
            r_high, r_low = split(right)
            image = dot(g_high, r_high) + (dot(g_low, r_high) + dot(g_high, r_low))
            rest = image - coef_ref[2 + step : 3 + step, :] * now
            if step:
                at = 2 + ITERS + step - 1
                rest = rest - coef_ref[at : at + 1, :] * basis_ref[step - 1]
            at = 2 + 2 * ITERS + step
            basis_ref[step + 1] = rest * coef_ref[at : at + 1, :]
        for other in range(step + 1):
            product = jnp.sum(basis_ref[other] * basis_ref[step], axis=0, keepdims=True)
            sums_ref[row : row + 1, :] = product[:, :TILE] + product[:, TILE:]
            row += 1
    ones = jnp.ones((TILE, TILE), F32)
    spread = jnp.dot(sums_ref[...], ones, preferred_element_type=F32, precision=lax.Precision.HIGHEST)
    r = lax.broadcasted_iota(jnp.int32, spread.shape, 0)
    c = lax.broadcasted_iota(jnp.int32, spread.shape, 1)
    packed = jnp.sum(jnp.where(r == c, spread, 0.0), axis=0, keepdims=True)
    inner_ref[...] = jnp.broadcast_to(packed[None], inner_ref.shape)


def basis_of(gram, coef, parts, devices):
    rank = gram.shape[0]
    return pl.pallas_call(
        basis_kernel,
        out_shape=(
            pltpu.VMEM((BASIS, rank, rank), F32),
            pltpu.VMEM((devices, 1, TILE), F32),
        ),
        in_specs=[IN_VMEM] * (2 + len(parts)),
        scratch_shapes=[pltpu.VMEM((PAIR_ROWS, TILE), F32)],
        compiler_params=LEAN,
        name="basis",
    )(*resident(gram, coef, *parts))


def tree(terms):
    terms = list(terms)
    while len(terms) > 1:
        terms = [sum(terms[i : i + 2][1:], terms[i]) for i in range(0, len(terms), 2)]
    return terms[0]


def solve_kernel(inner_ref, coef_ref, basis_ref, fit_ref, residual_ref, spread_ref):
    rank = basis_ref.shape[1]
    summed = jnp.sum(inner_ref[:, 0, :], axis=0, keepdims=True)
    r = lax.broadcasted_iota(jnp.int32, spread_ref.shape, 0)
    c = lax.broadcasted_iota(jnp.int32, spread_ref.shape, 1)
    alone = jnp.where(r == c, jnp.broadcast_to(summed, spread_ref.shape), 0.0)
    ones = jnp.ones((TILE, TILE), F32)
    spread_ref[...] = jnp.dot(alone, ones, preferred_element_type=F32, precision=lax.Precision.HIGHEST)

    def whole(value):
        return jnp.broadcast_to(value, (8, TILE))

    inner = {}
    for k, (i, j) in enumerate(PAIRS):
        inner[i, j] = inner[j, i] = whole(spread_ref[k : k + 1, :])
    norm2 = whole(coef_ref[1:2, :TILE])
    diagonal = [whole(coef_ref[2 + k : 3 + k, :TILE]) for k in range(ITERS)]
    off = [whole(coef_ref[2 + ITERS + k : 3 + ITERS + k, :TILE]) for k in range(ITERS)]

    def image(v):
        out = []
        for k in range(len(v) + 1):
            terms = []
            if k < len(v):
                terms.append(diagonal[k] * v[k])
            if k > 0:
                terms.append(off[k - 1] * v[k - 1])
            if k + 1 < len(v):
                terms.append(off[k] * v[k + 1])
            value = norm2 * tree(terms)
            out.append(value + RIDGE * v[k] if k < len(v) else value)
        return out

    def product(u, v):
        return tree([u[i] * tree([inner[i, j] * v[j] for j in range(len(v))]) for i in range(len(u))])

    one = jnp.ones((8, TILE), F32)
    residual = [one]
    direction = [one]
    fit = None
    norm_now = inner[0, 0]
    for step in range(ITERS):
        along = image(direction)
        size = norm_now / product(direction, along)
        if fit is None:
            fit = [size * direction[0]]
        else:
            fit = [f + size * d for f, d in zip(fit, direction)] + [size * direction[-1]]
        residual = [p - size * q for p, q in zip(residual, along)] + [-size * along[-1]]
        if step + 1 < ITERS:
            norm_next = product(residual, residual)
            ratio = norm_next / norm_now
            direction = [p + ratio * d for p, d in zip(residual, direction)] + [residual[-1]]
            norm_now = norm_next

    def lanes(value):
        return jnp.concatenate([value[0:1, :]] * (rank // TILE), axis=1)

    fit = [lanes(v) for v in fit]
    residual = [lanes(v) for v in residual]
    for top in range(0, rank, 32):
        at = slice(top, top + 32)
        parts = [basis_ref[k, at, :] for k in range(BASIS)]
        fit_ref[0, at, :] = tree([fit[k] * parts[k] for k in range(ITERS)])
        residual_ref[0, at, :] = tree([residual[k] * parts[k] for k in range(BASIS)])


def solve(inner, coef, basis):
    rank = basis.shape[1]
    return pl.pallas_call(
        solve_kernel,
        out_shape=(jax.ShapeDtypeStruct((1, rank, rank), F32),) * 2,
        in_specs=[IN_VMEM] * 3,
        scratch_shapes=[pltpu.VMEM((PAIR_ROWS, TILE), F32)],
        compiler_params=LEAN,
        name="solve",
    )(*resident(inner, coef, basis))


def shifted(array, bit):
    axes = ENT_BLK
    sizes = [lax.axis_size(a) for a in axes]
    pairs = []
    for x in range(sizes[0]):
        for core in range(sizes[1]):
            for y in range(sizes[2]):
                to = [x, core, y]
                if bit == "core":
                    to[1] ^= 1
                else:
                    near = bit[0] == "1"
                    axis = 0 if near == (core == 0) else 2
                    to[axis] ^= 1 if bit[1] == "e" else 3
                pairs.append(
                    ((x * sizes[1] + core) * sizes[2] + y, (to[0] * sizes[1] + to[1]) * sizes[2] + to[2])
                )
    return lax.ppermute(array, axes, pairs)


def gram_of(part):
    shards = lax.axis_size(ENT_BLK)
    rank = part.shape[0]
    pieces = lax.all_to_all(part.reshape(shards, rank // shards, rank), ENT_BLK, 0, 0, tiled=True)
    own = jnp.sum(pieces, axis=0)
    return lax.all_to_all(
        jnp.broadcast_to(own[None], (shards, *own.shape)), ENT_BLK, 0, 0, tiled=True
    ).reshape(rank, rank)


def body(factors, heads, tails, values):
    shards = lax.axis_size(ENT_BLK)
    ent_dev = factors.shape[0]
    width = heads.shape[3]
    relations = heads.shape[0] * heads.shape[2]
    scale = 1.0 / math.sqrt(shards * width)
    heads = heads.reshape(relations, 1, width)
    tails = tails.reshape(relations, 1, width)
    values = values.reshape(relations, 1, width)
    x, core, y = (lax.axis_index(a) for a in ENT_BLK)
    rows = lax.axis_size("blk")

    def order(of_core, first):
        second = jnp.arange(rows, dtype=jnp.int32)[None]
        first = jnp.asarray(first, jnp.int32)[:, None]
        to_x = x ^ jnp.where(of_core == 0, first, second)
        to_y = y ^ jnp.where(of_core == 0, second, first)
        return (to_x * 2 + of_core) * rows + to_y

    firsts = (2, 1, 3, 0)
    orders = jnp.concatenate([order(1 - core, firsts), order(core, firsts)]).astype(jnp.int32)
    heads, tails, values = resident(heads, tails, values)
    table, gram_part = tables(factors)
    (table,) = resident(table)
    gram = gram_of(gram_part) / (ent_dev * shards)
    coef = recurrence(gram)

    sums = functools.partial(
        triple_sums, order=orders, heads=heads, tails=tails, values=values, table=table, scale=scale
    )
    upper, lower = {}, {}
    from_partner = {}
    for k, first in enumerate(firsts):
        from_partner[first] = shifted(sums(k), "core")
    for k, first in enumerate(firsts):
        upper[first], lower[first] = sums(len(firsts) + k, partner=from_partner[first])

    up2 = shifted(upper[2], "1e")
    low2 = shifted(lower[2], "1o")
    up1 = shifted(upper[1], "1e")
    low3 = shifted(lower[3], "1o")
    up_b = shifted(upper[3] + up2, "1o")
    low_b = shifted(lower[1] + low2, "1e")
    up_c = shifted(upper[0][1:3] + up1[1:3] + up_b[1:3], "2e")
    low_c = shifted(lower[0][2:4] + low3[2:4] + low_b[2:4], "2o")
    up_d = shifted(upper[0][3] + up1[3] + up_b[3] + up_c[1], "2o")
    low_d = shifted(lower[0][1] + low3[1] + low_b[1] + low_c[0], "2e")
    up_own = upper[0][0] + up1[0] + up_b[0] + up_c[0]
    low_own = lower[0][0] + low3[0] + low_b[0] + low_c[1]

    devices = lax.axis_size(ENT_BLK_REL)
    basis, inner = basis_of(gram, coef, (up_own, up_d, low_own, low_d), devices)
    inner = lax.all_to_all(inner, ENT_BLK_REL, 0, 0, tiled=True)
    return solve(inner, coef, basis)


def solution(mesh):
    torus = Mesh(
        mesh.devices.reshape(mesh.shape["ent"] // 2, 2, mesh.shape["blk"], mesh.shape["rel"]),
        ENT_BLK_REL,
    )
    spread = P(None, "rel", None, ENT_BLK)
    whole = P(ENT_BLK_REL, None, None)
    return jax.shard_map(
        body,
        mesh=torus,
        in_specs=(P(ENT_BLK, None), spread, spread, spread),
        out_specs=(whole, whole),
        check_vma=False,
    )
```

```python
import functools
import math

import jax
import jax.numpy as jnp
from jax import lax
from jax.experimental import pallas as pl
from jax.experimental.pallas import tpu as pltpu
from jax.sharding import Mesh
from jax.sharding import PartitionSpec as P

F32 = jnp.float32
BF16 = jnp.bfloat16
ITERS = 8
TILE = 128
RIDGE = 0.01
TINY = 1e-12
ENT_BLK_REL = ("ent_0", "ent_1", "blk", "rel")
ENT_BLK = ("ent_0", "ent_1", "blk")
BASIS = ITERS + 1
PAIRS = [(i, j) for j in range(BASIS) for i in range(j + 1)]
PAIR_ROWS = -(-len(PAIRS) // 8) * 8


def tables_kernel(
    factors_hbm, heads_hbm, tails_hbm, values_hbm, table_ref, gram_ref, heads_ref, tails_ref, values_ref, factors_ref, sems
):
    sources = (factors_hbm, heads_hbm, tails_hbm, values_hbm)
    targets = (factors_ref, heads_ref, tails_ref, values_ref)
    copies = [pltpu.make_async_copy(s, t, sems.at[k]) for k, (s, t) in enumerate(zip(sources, targets))]
    for copy in copies:
        copy.start()
    copies[0].wait()
    gram = None
    for b in range(factors_ref.shape[0] // TILE):
        rows = factors_ref[b * TILE : (b + 1) * TILE, :]
        columns = rows.astype(F32).T
        table_ref[b] = columns
        part = jnp.dot(columns.astype(BF16), rows, preferred_element_type=F32)
        gram = part if gram is None else gram + part
    half = gram.shape[0] // 2
    gram_ref[:half] = gram[:half, :half]
    gram_ref[half : 2 * half] = gram[:half, half:]
    gram_ref[2 * half :] = gram[half:, half:]
    for copy in copies[1:]:
        copy.wait()


def resident(*arrays):
    return tuple(pltpu.with_memory_space_constraint(a, pltpu.VMEM) for a in arrays)


LEAN = pltpu.CompilerParams(vmem_limit_bytes=16 * 2**20)


def cost(products, moved=0):
    return pl.CostEstimate(flops=products * 2 * 256**3, bytes_accessed=moved, transcendentals=0)


IN_VMEM = pl.BlockSpec(memory_space=pltpu.VMEM)
IN_SMEM = pl.BlockSpec(memory_space=pltpu.SMEM)


def tables(factors, heads, tails, values):
    ents, rank = factors.shape
    return pl.pallas_call(
        tables_kernel,
        in_specs=[pl.BlockSpec(memory_space=pltpu.HBM)] * 4,
        out_shape=(
            pltpu.VMEM((ents // TILE, rank, TILE), F32),
            pltpu.VMEM((3 * rank // 2, rank // 2), F32),
            pltpu.VMEM(heads.shape, jnp.int32),
            pltpu.VMEM(tails.shape, jnp.int32),
            pltpu.VMEM(values.shape, F32),
        ),
        scratch_shapes=[pltpu.VMEM(factors.shape, BF16), pltpu.SemaphoreType.DMA((4,))],
        compiler_params=LEAN,
        name="tables",
    )(*(pltpu.with_memory_space_constraint(a, pltpu.HBM) for a in (factors, heads, tails, values)))


def square_of(packed, ents):
    half = packed.shape[1]
    packed = packed * (1.0 / ents)
    corner = packed[half : 2 * half]
    upper = jnp.concatenate([packed[:half], corner], axis=1)
    lower = jnp.concatenate([corner.T, packed[2 * half :]], axis=1)
    return jnp.concatenate([upper, lower], axis=0)


def lane_pick(block, ids):
    dims = lax.GatherDimensionNumbers(
        offset_dims=(),
        collapsed_slice_dims=(1,),
        start_index_map=(1,),
        operand_batching_dims=(0,),
        start_indices_batching_dims=(0,),
    )
    return lax.gather(
        block, ids[..., None], dims, (1, 1), mode=lax.GatherScatterMode.PROMISE_IN_BOUNDS
    )


def triple_kernel(heads_ref, tails_ref, values_ref, table_ref, *rest, first, scale, halves):
    if halves:
        partner_ref, upper_ref, lower_ref = rest[-3:]
    else:
        out_ref = rest[-1]
    rank = table_ref.shape[1]
    width = heads_ref.shape[2]
    x, core, y = (lax.axis_index(a) for a in ENT_BLK)
    to_core = core if halves else 1 - core
    columns = lax.axis_size("blk")

    def rows(ids_ref, relation, tile):
        at = slice(tile * TILE, (tile + 1) * TILE)
        block = ids_ref[relation, 0, tile * TILE] // TILE
        inside = jnp.broadcast_to(ids_ref[relation, :, at] & (TILE - 1), (rank, TILE))
        return lane_pick(table_ref[block], inside).astype(BF16)

    for i in range(columns):
        to_x = x ^ jnp.where(to_core == 0, first, i)
        to_y = y ^ jnp.where(to_core == 0, i, first)
        relation = (to_x * 2 + to_core) * columns + to_y
        summed = None
        for pair in range(0, width // TILE, 2):
            tiles = range(pair, min(pair + 2, width // TILE))
            weighted = []
            for tile in tiles:
                at = slice(tile * TILE, (tile + 1) * TILE)
                head_rows = rows(heads_ref, relation, tile).astype(F32)
                weighted.append((head_rows * values_ref[relation, :, at]).astype(BF16))
            weighted = jnp.concatenate(weighted, axis=1)
            tail_rows = jnp.concatenate([rows(tails_ref, relation, tile) for tile in tiles], axis=1)
            part = lax.dot_general(
                weighted, tail_rows, (((1,), (1,)), ((), ())), preferred_element_type=F32
            )
            summed = part if summed is None else summed + part
        summed = summed * scale
        if halves:
            summed = summed + partner_ref[i]
            upper_ref[i] = summed[: rank // 2]
            lower_ref[i] = summed[rank // 2 :]
        else:
            out_ref[i] = summed


def triple_sums(first, heads, tails, values, table, scale, partner=None, after=None):
    count = lax.axis_size("blk")
    width = heads.shape[2]
    rank = table.shape[1]
    args = [heads, tails, values, table]
    if after is not None:
        args.append(after)
    if partner is None:
        shape = pltpu.VMEM((count, rank, rank), F32)
    else:
        args.append(partner)
        shape = (pltpu.VMEM((count, rank // 2, rank), F32),) * 2
    return pl.pallas_call(
        functools.partial(triple_kernel, first=first, scale=scale, halves=partner is not None),
        in_specs=[IN_VMEM] * len(args),
        out_shape=shape,
        compiler_params=LEAN,
        cost_estimate=cost(count * width // 256),
    )(*resident(*args))


def total(array):
    return jnp.sum(jnp.sum(array, axis=0, keepdims=True), axis=1, keepdims=True)


def split(array):
    high = array.astype(BF16)
    return high, (array - high.astype(F32)).astype(BF16)


def dot(a, b):
    return jnp.dot(a, b, preferred_element_type=F32)


def signs(rank):
    i = lax.broadcasted_iota(jnp.int32, (rank, rank), 0)
    j = lax.broadcasted_iota(jnp.int32, (rank, rank), 1)
    mixed = i * 40503 + j * 30011 + 12345
    for step in (7, 3):
        mixed = mixed ^ lax.shift_right_logical(mixed, jnp.full_like(mixed, step * 2))
        mixed = mixed * 739982445
    mixed = mixed ^ lax.shift_right_logical(mixed, jnp.full_like(mixed, 15))
    return jnp.where((mixed & 64) == 0, 1.0, -1.0).astype(F32)


def basis_kernel(gram_ref, ua_ref, ub_ref, la_ref, lb_ref, basis_ref, inner_ref, coef_ref, sums_ref, *, ents):
    gram = square_of(gram_ref[...], ents)
    rank = gram.shape[0]
    half = rank // 2
    basis_ref[0, :half, :] = ua_ref[...] + ub_ref[...]
    basis_ref[0, half:, :] = la_ref[...] + lb_ref[...]
    sums_ref[...] = jnp.zeros_like(sums_ref)
    norm2 = total(gram * gram)
    inverse = lax.rsqrt(norm2)
    g_high, g_low = split(gram * inverse)

    def rough(v):
        return dot(g_high, dot(v.astype(BF16), g_high).astype(BF16))

    def put(row, value):
        coef_ref[row : row + 1, :] = jnp.broadcast_to(value, (1, rank))

    put(0, norm2)
    now = signs(rank)
    ahead = rough(now)
    size = lax.rsqrt(jnp.maximum(total(now * ahead), TINY))
    now = now * size
    ahead = ahead * size
    before = None
    behind = None
    off = None
    row = 0
    for step in range(BASIS):
        vector = basis_ref[step]
        if step < ITERS:
            v_high, v_low = split(vector)
            right = dot(v_high, g_high) + (dot(v_low, g_high) + dot(v_high, g_low))
            next_image = rough(ahead)
            r_high, r_low = split(right)
            image = dot(g_high, r_high) + (dot(g_low, r_high) + dot(g_high, r_low))
            diagonal = total(ahead * ahead)
            rest = ahead - diagonal * now
            rest_image = next_image - diagonal * ahead
            image = image - diagonal * vector
            if step:
                rest = rest - off * before
                rest_image = rest_image - off * behind
                image = image - off * basis_ref[step - 1]
            square = jnp.maximum(total(rest * rest_image), TINY)
            inverse_off = lax.rsqrt(square)
            off = square * inverse_off
            put(1 + step, diagonal)
            put(1 + ITERS + step, off)
            basis_ref[step + 1] = image * inverse_off
            before = now
            behind = ahead
            now = rest * inverse_off
            ahead = rest_image * inverse_off
        for other in range(step + 1):
            product = jnp.sum(basis_ref[other] * vector, axis=0, keepdims=True)
            sums_ref[row : row + 1, :] = product[:, :TILE] + product[:, TILE:]
            row += 1
    ones = jnp.ones((TILE, TILE), F32)
    spread = jnp.dot(sums_ref[...], ones, preferred_element_type=F32, precision=lax.Precision.HIGHEST)
    r = lax.broadcasted_iota(jnp.int32, spread.shape, 0)
    c = lax.broadcasted_iota(jnp.int32, spread.shape, 1)
    packed = jnp.sum(jnp.where(r == c, spread, 0.0), axis=0, keepdims=True)
    inner_ref[...] = jnp.broadcast_to(packed[None], inner_ref.shape)


COEF_ROWS = -(-(1 + 2 * ITERS) // 8) * 8


def basis_of(gram, parts, devices, ents):
    rank = 2 * gram.shape[1]
    return pl.pallas_call(
        functools.partial(basis_kernel, ents=ents),
        out_shape=(
            pltpu.VMEM((BASIS, rank, rank), F32),
            pltpu.VMEM((devices, 1, TILE), F32),
            pltpu.VMEM((COEF_ROWS, rank), F32),
        ),
        in_specs=[IN_VMEM] * (1 + len(parts)),
        scratch_shapes=[pltpu.VMEM((PAIR_ROWS, TILE), F32)],
        compiler_params=LEAN,
        cost_estimate=cost(8 * ITERS),
        name="basis",
    )(*resident(gram, *parts))


def tree(terms):
    terms = list(terms)
    while len(terms) > 1:
        terms = [sum(terms[i : i + 2][1:], terms[i]) for i in range(0, len(terms), 2)]
    return terms[0]


def solve_kernel(inner_ref, coef_ref, basis_ref, fit_ref, residual_ref, spread_ref):
    rank = basis_ref.shape[1]
    summed = jnp.sum(inner_ref[:, 0, :], axis=0, keepdims=True)
    r = lax.broadcasted_iota(jnp.int32, spread_ref.shape, 0)
    c = lax.broadcasted_iota(jnp.int32, spread_ref.shape, 1)
    alone = jnp.where(r == c, jnp.broadcast_to(summed, spread_ref.shape), 0.0)
    ones = jnp.ones((TILE, TILE), F32)
    spread_ref[...] = jnp.dot(alone, ones, preferred_element_type=F32, precision=lax.Precision.HIGHEST)

    def whole(value):
        return jnp.broadcast_to(value, (8, TILE))

    inner = {}
    for k, (i, j) in enumerate(PAIRS):
        inner[i, j] = inner[j, i] = whole(spread_ref[k : k + 1, :])
    norm2 = whole(coef_ref[0:1, :TILE])
    diagonal = [whole(coef_ref[1 + k : 2 + k, :TILE]) for k in range(ITERS)]
    off = [whole(coef_ref[1 + ITERS + k : 2 + ITERS + k, :TILE]) for k in range(ITERS)]

    def image(v):
        out = []
        for k in range(len(v) + 1):
            terms = []
            if k < len(v):
                terms.append(diagonal[k] * v[k])
            if k > 0:
                terms.append(off[k - 1] * v[k - 1])
            if k + 1 < len(v):
                terms.append(off[k] * v[k + 1])
            value = norm2 * tree(terms)
            out.append(value + RIDGE * v[k] if k < len(v) else value)
        return out

    def product(u, v):
        return tree([u[i] * tree([inner[i, j] * v[j] for j in range(len(v))]) for i in range(len(u))])

    one = jnp.ones((8, TILE), F32)
    residual = [one]
    direction = [one]
    fit = None
    norm_now = inner[0, 0]
    for step in range(ITERS):
        along = image(direction)
        size = norm_now / product(direction, along)
        if fit is None:
            fit = [size * direction[0]]
        else:
            fit = [f + size * d for f, d in zip(fit, direction)] + [size * direction[-1]]
        residual = [p - size * q for p, q in zip(residual, along)] + [-size * along[-1]]
        if step + 1 < ITERS:
            norm_next = product(residual, residual)
            ratio = norm_next / norm_now
            direction = [p + ratio * d for p, d in zip(residual, direction)] + [residual[-1]]
            norm_now = norm_next

    def lanes(value):
        return jnp.concatenate([value[0:1, :]] * (rank // TILE), axis=1)

    fit = [lanes(v) for v in fit]
    residual = [lanes(v) for v in residual]
    for top in range(0, rank, 32):
        at = slice(top, top + 32)
        parts = [basis_ref[k, at, :] for k in range(BASIS)]
        fit_ref[0, at, :] = tree([fit[k] * parts[k] for k in range(ITERS)])
        residual_ref[0, at, :] = tree([residual[k] * parts[k] for k in range(BASIS)])


def solve(inner, coef, basis):
    rank = basis.shape[1]
    return pl.pallas_call(
        solve_kernel,
        out_shape=(jax.ShapeDtypeStruct((1, rank, rank), F32),) * 2,
        in_specs=[IN_VMEM] * 3,
        scratch_shapes=[pltpu.VMEM((PAIR_ROWS, TILE), F32)],
        compiler_params=LEAN,
        name="solve",
    )(*resident(inner, coef, basis))


def shifted(array, bit):
    axes = ENT_BLK
    sizes = [lax.axis_size(a) for a in axes]
    pairs = []
    for x in range(sizes[0]):
        for core in range(sizes[1]):
            for y in range(sizes[2]):
                to = [x, core, y]
                if bit == "core":
                    to[1] ^= 1
                else:
                    near = bit[0] == "1"
                    axis = 0 if near == (core == 0) else 2
                    to[axis] ^= 1 if bit[1] == "e" else 3
                pairs.append(
                    ((x * sizes[1] + core) * sizes[2] + y, (to[0] * sizes[1] + to[1]) * sizes[2] + to[2])
                )
    return lax.ppermute(array, axes, pairs)


def fit(factors, heads, tails, values):
    shards = lax.axis_size(ENT_BLK)
    ent_dev = factors.shape[0]
    width = heads.shape[3]
    relations = heads.shape[0] * heads.shape[2]
    scale = 1.0 / math.sqrt(shards * width)
    heads = heads.reshape(relations, 1, width)
    tails = tails.reshape(relations, 1, width)
    values = values.reshape(relations, 1, width)
    ents = ent_dev * shards
    table, gram_part, heads, tails, values = tables(factors, heads, tails, values)
    gram = gram_part
    for bit in ("core", "1e", "1o", "2e", "2o"):
        gram = gram + shifted(gram, bit)
    sums = functools.partial(
        triple_sums, heads=heads, tails=tails, values=values, table=table, scale=scale
    )
    upper, lower = {}, {}
    from_partner = {}

    def give(first, after=None):
        partial = sums(first, after=after)
        from_partner[first] = shifted(partial, "core")
        return partial

    def keep(first, after=None):
        upper[first], lower[first] = sums(first, partner=from_partner[first], after=after)

    give(2)
    give(1)
    keep(2)
    third = give(3, upper[2])
    keep(1, third)
    keep(3, upper[1])
    give(0, upper[3])
    keep(0)

    up2 = shifted(upper[2], "1e")
    low2 = shifted(lower[2], "1o")
    up1 = shifted(upper[1], "1e")
    low3 = shifted(lower[3], "1o")
    up_b = shifted(upper[3] + up2, "1o")
    low_b = shifted(lower[1] + low2, "1e")
    up_c = upper[0][1:3] + up1[1:3] + up_b[1:3]
    low_c = lower[0][2:4] + low3[2:4] + low_b[2:4]
    up_c = shifted(up_c, "2e")
    low_c = shifted(low_c, "2o")
    up_d = shifted(upper[0][3] + up1[3] + up_b[3] + up_c[1], "2o")
    low_d = shifted(lower[0][1] + low3[1] + low_b[1] + low_c[0], "2e")
    up_own = upper[0][0] + up1[0] + up_b[0] + up_c[0]
    low_own = lower[0][0] + low3[0] + low_b[0] + low_c[1]

    devices = lax.axis_size(ENT_BLK_REL)
    basis, inner, coef = basis_of(gram, (up_own, up_d, low_own, low_d), devices, ents)
    inner = lax.all_to_all(inner, ENT_BLK_REL, 0, 0, tiled=True)
    return solve(inner, coef, basis)


def solution(mesh):
    torus = Mesh(
        mesh.devices.reshape(mesh.shape["ent"] // 2, 2, mesh.shape["blk"], mesh.shape["rel"]),
        ENT_BLK_REL,
    )
    spread = P(None, "rel", None, ENT_BLK)
    whole = P(ENT_BLK_REL, None, None)
    return jax.shard_map(
        fit,
        mesh=torus,
        in_specs=(P(ENT_BLK, None), spread, spread, spread),
        out_specs=(whole, whole),
        check_vma=False,
    )
```

```python
import functools
import math

import jax
import jax.numpy as jnp
from jax import lax
from jax.experimental import pallas as pl
from jax.experimental.pallas import tpu as pltpu
from jax.sharding import Mesh
from jax.sharding import PartitionSpec as P

F32 = jnp.float32
BF16 = jnp.bfloat16
ITERS = 8
TILE = 128
RIDGE = 0.01
TINY = 1e-12
ENT_BLK_REL = ("ent_0", "ent_1", "blk", "rel")
ENT_BLK = ("ent_0", "ent_1", "blk")
BASIS = ITERS + 1
PAIRS = [(i, j) for j in range(BASIS) for i in range(j + 1)]
PAIR_ROWS = -(-len(PAIRS) // 8) * 8


def tables_kernel(
    factors_hbm, heads_hbm, tails_hbm, values_hbm, table_ref, gram_ref, heads_ref, tails_ref, values_ref, factors_ref, sems
):
    sources = (factors_hbm, heads_hbm, tails_hbm, values_hbm)
    targets = (factors_ref, heads_ref, tails_ref, values_ref)
    copies = [pltpu.make_async_copy(s, t, sems.at[k]) for k, (s, t) in enumerate(zip(sources, targets))]
    for copy in copies:
        copy.start()
    copies[0].wait()
    gram = None
    for b in range(factors_ref.shape[0] // TILE):
        rows = factors_ref[b * TILE : (b + 1) * TILE, :]
        columns = rows.astype(F32).T
        table_ref[b] = columns
        part = jnp.dot(columns.astype(BF16), rows, preferred_element_type=F32)
        gram = part if gram is None else gram + part
    half = gram.shape[0] // 2
    gram_ref[:half] = gram[:half, :half]
    gram_ref[half : 2 * half] = gram[:half, half:]
    gram_ref[2 * half :] = gram[half:, half:]
    for copy in copies[1:]:
        copy.wait()


def resident(*arrays):
    return tuple(pltpu.with_memory_space_constraint(a, pltpu.VMEM) for a in arrays)


LEAN = pltpu.CompilerParams(vmem_limit_bytes=16 * 2**20)


def cost(products, moved=0):
    return pl.CostEstimate(flops=products * 2 * 256**3, bytes_accessed=moved, transcendentals=0)


IN_VMEM = pl.BlockSpec(memory_space=pltpu.VMEM)
IN_SMEM = pl.BlockSpec(memory_space=pltpu.SMEM)


def tables(factors, heads, tails, values):
    ents, rank = factors.shape
    return pl.pallas_call(
        tables_kernel,
        in_specs=[pl.BlockSpec(memory_space=pltpu.HBM)] * 4,
        out_shape=(
            pltpu.VMEM((ents // TILE, rank, TILE), F32),
            pltpu.VMEM((3 * rank // 2, rank // 2), F32),
            pltpu.VMEM(heads.shape, jnp.int32),
            pltpu.VMEM(tails.shape, jnp.int32),
            pltpu.VMEM(values.shape, F32),
        ),
        scratch_shapes=[pltpu.VMEM(factors.shape, BF16), pltpu.SemaphoreType.DMA((4,))],
        compiler_params=LEAN,
        name="tables",
    )(*(pltpu.with_memory_space_constraint(a, pltpu.HBM) for a in (factors, heads, tails, values)))


def square_of(packed, ents):
    half = packed.shape[1]
    packed = packed * (1.0 / ents)
    corner = packed[half : 2 * half]
    upper = jnp.concatenate([packed[:half], corner], axis=1)
    lower = jnp.concatenate([corner.T, packed[2 * half :]], axis=1)
    return jnp.concatenate([upper, lower], axis=0)


def lane_pick(block, ids):
    dims = lax.GatherDimensionNumbers(
        offset_dims=(),
        collapsed_slice_dims=(1,),
        start_index_map=(1,),
        operand_batching_dims=(0,),
        start_indices_batching_dims=(0,),
    )
    return lax.gather(
        block, ids[..., None], dims, (1, 1), mode=lax.GatherScatterMode.PROMISE_IN_BOUNDS
    )


def triple_kernel(heads_ref, tails_ref, values_ref, table_ref, *rest, first, scale, halves):
    if halves:
        partner_ref, upper_ref, lower_ref = rest[-3:]
    else:
        out_ref = rest[-1]
    rank = table_ref.shape[1]
    width = heads_ref.shape[2]
    x, core, y = (lax.axis_index(a) for a in ENT_BLK)
    to_core = core if halves else 1 - core
    columns = lax.axis_size("blk")

    def rows(ids_ref, relation, tile):
        at = slice(tile * TILE, (tile + 1) * TILE)
        block = ids_ref[relation, 0, tile * TILE] // TILE
        inside = jnp.broadcast_to(ids_ref[relation, :, at] & (TILE - 1), (rank, TILE))
        return lane_pick(table_ref[block], inside).astype(BF16)

    def rows_by_product(ids_ref, relation, tiles):
        place = lax.broadcasted_iota(jnp.int32, (TILE, TILE), 0)
        nothing = jnp.zeros((TILE, TILE), BF16)
        blocks, picks = [], []
        for tile in tiles:
            at = slice(tile * TILE, (tile + 1) * TILE)
            block = ids_ref[relation, 0, tile * TILE] // TILE
            inside = ids_ref[relation, :, at] & (TILE - 1)
            blocks.append(table_ref[block].astype(BF16))
            picks.append(jnp.where(place == inside, 1.0, 0.0).astype(BF16))
        pick = jnp.concatenate(
            [jnp.concatenate([picks[0], nothing], axis=1), jnp.concatenate([nothing, picks[1]], axis=1)], axis=0
        )
        return dot(jnp.concatenate(blocks, axis=1), pick).astype(BF16)

    by_product = (0, 6)
    for i in range(columns):
        to_x = x ^ jnp.where(to_core == 0, first, i)
        to_y = y ^ jnp.where(to_core == 0, i, first)
        relation = (to_x * 2 + to_core) * columns + to_y
        summed = None
        for pair in range(0, width // TILE, 2):
            tiles = range(pair, min(pair + 2, width // TILE))
            weighted = []
            for tile in tiles:
                at = slice(tile * TILE, (tile + 1) * TILE)
                head_rows = rows(heads_ref, relation, tile).astype(F32)
                weighted.append((head_rows * values_ref[relation, :, at]).astype(BF16))
            weighted = jnp.concatenate(weighted, axis=1)
            if pair in by_product and len(tiles) == 2:
                tail_rows = rows_by_product(tails_ref, relation, tiles)
            else:
                tail_rows = jnp.concatenate([rows(tails_ref, relation, tile) for tile in tiles], axis=1)
            part = lax.dot_general(
                weighted, tail_rows, (((1,), (1,)), ((), ())), preferred_element_type=F32
            )
            summed = part if summed is None else summed + part
        summed = summed * scale
        if halves:
            summed = summed + partner_ref[i]
            upper_ref[i] = summed[: rank // 2]
            lower_ref[i] = summed[rank // 2 :]
        else:
            out_ref[i] = summed


def triple_sums(first, heads, tails, values, table, scale, partner=None, after=None):
    count = lax.axis_size("blk")
    width = heads.shape[2]
    rank = table.shape[1]
    args = [heads, tails, values, table]
    if after is not None:
        args.append(after)
    if partner is None:
        shape = pltpu.VMEM((count, rank, rank), F32)
    else:
        args.append(partner)
        shape = (pltpu.VMEM((count, rank // 2, rank), F32),) * 2
    return pl.pallas_call(
        functools.partial(triple_kernel, first=first, scale=scale, halves=partner is not None),
        in_specs=[IN_VMEM] * len(args),
        out_shape=shape,
        compiler_params=LEAN,
        cost_estimate=cost(count * width // 256),
    )(*resident(*args))


def total(array):
    return jnp.sum(jnp.sum(array, axis=0, keepdims=True), axis=1, keepdims=True)


def split(array):
    high = array.astype(BF16)
    return high, (array - high.astype(F32)).astype(BF16)


def dot(a, b):
    return jnp.dot(a, b, preferred_element_type=F32)


def signs(rank):
    i = lax.broadcasted_iota(jnp.int32, (rank, rank), 0)
    j = lax.broadcasted_iota(jnp.int32, (rank, rank), 1)
    mixed = i * 40503 + j * 30011 + 12345
    for step in (7, 3):
        mixed = mixed ^ lax.shift_right_logical(mixed, jnp.full_like(mixed, step * 2))
        mixed = mixed * 739982445
    mixed = mixed ^ lax.shift_right_logical(mixed, jnp.full_like(mixed, 15))
    return jnp.where((mixed & 64) == 0, 1.0, -1.0).astype(F32)


def basis_kernel(gram_ref, ua_ref, ub_ref, la_ref, lb_ref, basis_ref, inner_ref, coef_ref, sums_ref, *, ents):
    gram = square_of(gram_ref[...], ents)
    rank = gram.shape[0]
    half = rank // 2
    basis_ref[0, :half, :] = ua_ref[...] + ub_ref[...]
    basis_ref[0, half:, :] = la_ref[...] + lb_ref[...]
    sums_ref[...] = jnp.zeros_like(sums_ref)
    norm2 = total(gram * gram)
    inverse = lax.rsqrt(norm2)
    g_high, g_low = split(gram * inverse)

    def rough(v):
        return dot(g_high, dot(v.astype(BF16), g_high).astype(BF16))

    def put(row, value):
        coef_ref[row : row + 1, :] = jnp.broadcast_to(value, (1, rank))

    put(0, norm2)
    now = signs(rank)
    ahead = rough(now)
    size = lax.rsqrt(jnp.maximum(total(now * ahead), TINY))
    now = now * size
    ahead = ahead * size
    before = None
    behind = None
    off = None
    row = 0
    for step in range(BASIS):
        vector = basis_ref[step]
        if step < ITERS:
            v_high, v_low = split(vector)
            right = dot(v_high, g_high) + (dot(v_low, g_high) + dot(v_high, g_low))
            next_image = rough(ahead)
            r_high, r_low = split(right)
            image = dot(g_high, r_high) + (dot(g_low, r_high) + dot(g_high, r_low))
            diagonal = total(ahead * ahead)
            rest = ahead - diagonal * now
            rest_image = next_image - diagonal * ahead
            image = image - diagonal * vector
            if step:
                rest = rest - off * before
                rest_image = rest_image - off * behind
                image = image - off * basis_ref[step - 1]
            square = jnp.maximum(total(rest * rest_image), TINY)
            inverse_off = lax.rsqrt(square)
            off = square * inverse_off
            put(1 + step, diagonal)
            put(1 + ITERS + step, off)
            basis_ref[step + 1] = image * inverse_off
            before = now
            behind = ahead
            now = rest * inverse_off
            ahead = rest_image * inverse_off
        for other in range(step + 1):
            product = jnp.sum(basis_ref[other] * vector, axis=0, keepdims=True)
            sums_ref[row : row + 1, :] = product[:, :TILE] + product[:, TILE:]
            row += 1
    ones = jnp.ones((TILE, TILE), F32)
    spread = jnp.dot(sums_ref[...], ones, preferred_element_type=F32, precision=lax.Precision.HIGHEST)
    r = lax.broadcasted_iota(jnp.int32, spread.shape, 0)
    c = lax.broadcasted_iota(jnp.int32, spread.shape, 1)
    packed = jnp.sum(jnp.where(r == c, spread, 0.0), axis=0, keepdims=True)
    inner_ref[...] = jnp.broadcast_to(packed[None], inner_ref.shape)


COEF_ROWS = -(-(1 + 2 * ITERS) // 8) * 8


def basis_of(gram, parts, devices, ents):
    rank = 2 * gram.shape[1]
    return pl.pallas_call(
        functools.partial(basis_kernel, ents=ents),
        out_shape=(
            pltpu.VMEM((BASIS, rank, rank), F32),
            pltpu.VMEM((devices, 1, TILE), F32),
            pltpu.VMEM((COEF_ROWS, rank), F32),
        ),
        in_specs=[IN_VMEM] * (1 + len(parts)),
        scratch_shapes=[pltpu.VMEM((PAIR_ROWS, TILE), F32)],
        compiler_params=LEAN,
        cost_estimate=cost(8 * ITERS),
        name="basis",
    )(*resident(gram, *parts))


def tree(terms):
    terms = list(terms)
    while len(terms) > 1:
        terms = [sum(terms[i : i + 2][1:], terms[i]) for i in range(0, len(terms), 2)]
    return terms[0]


def solve_kernel(inner_ref, coef_ref, basis_ref, fit_ref, residual_ref, spread_ref):
    rank = basis_ref.shape[1]
    summed = jnp.sum(inner_ref[:, 0, :], axis=0, keepdims=True)
    r = lax.broadcasted_iota(jnp.int32, spread_ref.shape, 0)
    c = lax.broadcasted_iota(jnp.int32, spread_ref.shape, 1)
    alone = jnp.where(r == c, jnp.broadcast_to(summed, spread_ref.shape), 0.0)
    ones = jnp.ones((TILE, TILE), F32)
    spread_ref[...] = jnp.dot(alone, ones, preferred_element_type=F32, precision=lax.Precision.HIGHEST)

    def whole(value):
        return jnp.broadcast_to(value, (8, TILE))

    inner = {}
    for k, (i, j) in enumerate(PAIRS):
        inner[i, j] = inner[j, i] = whole(spread_ref[k : k + 1, :])
    norm2 = whole(coef_ref[0:1, :TILE])
    diagonal = [whole(coef_ref[1 + k : 2 + k, :TILE]) for k in range(ITERS)]
    off = [whole(coef_ref[1 + ITERS + k : 2 + ITERS + k, :TILE]) for k in range(ITERS)]

    def image(v):
        out = []
        for k in range(len(v) + 1):
            terms = []
            if k < len(v):
                terms.append(diagonal[k] * v[k])
            if k > 0:
                terms.append(off[k - 1] * v[k - 1])
            if k + 1 < len(v):
                terms.append(off[k] * v[k + 1])
            value = norm2 * tree(terms)
            out.append(value + RIDGE * v[k] if k < len(v) else value)
        return out

    def product(u, v):
        return tree([u[i] * tree([inner[i, j] * v[j] for j in range(len(v))]) for i in range(len(u))])

    one = jnp.ones((8, TILE), F32)
    residual = [one]
    direction = [one]
    fit = None
    norm_now = inner[0, 0]
    for step in range(ITERS):
        along = image(direction)
        size = norm_now / product(direction, along)
        if fit is None:
            fit = [size * direction[0]]
        else:
            fit = [f + size * d for f, d in zip(fit, direction)] + [size * direction[-1]]
        residual = [p - size * q for p, q in zip(residual, along)] + [-size * along[-1]]
        if step + 1 < ITERS:
            norm_next = product(residual, residual)
            ratio = norm_next / norm_now
            direction = [p + ratio * d for p, d in zip(residual, direction)] + [residual[-1]]
            norm_now = norm_next

    def lanes(value):
        return jnp.concatenate([value[0:1, :]] * (rank // TILE), axis=1)

    fit = [lanes(v) for v in fit]
    residual = [lanes(v) for v in residual]
    for top in range(0, rank, 32):
        at = slice(top, top + 32)
        parts = [basis_ref[k, at, :] for k in range(BASIS)]
        fit_ref[0, at, :] = tree([fit[k] * parts[k] for k in range(ITERS)])
        residual_ref[0, at, :] = tree([residual[k] * parts[k] for k in range(BASIS)])


def solve(inner, coef, basis):
    rank = basis.shape[1]
    return pl.pallas_call(
        solve_kernel,
        out_shape=(jax.ShapeDtypeStruct((1, rank, rank), F32),) * 2,
        in_specs=[IN_VMEM] * 3,
        scratch_shapes=[pltpu.VMEM((PAIR_ROWS, TILE), F32)],
        compiler_params=LEAN,
        name="solve",
    )(*resident(inner, coef, basis))


def shifted(array, bit):
    axes = ENT_BLK
    sizes = [lax.axis_size(a) for a in axes]
    pairs = []
    for x in range(sizes[0]):
        for core in range(sizes[1]):
            for y in range(sizes[2]):
                to = [x, core, y]
                if bit == "core":
                    to[1] ^= 1
                else:
                    near = bit[0] == "1"
                    axis = 0 if near == (core == 0) else 2
                    to[axis] ^= 1 if bit[1] == "e" else 3
                pairs.append(
                    ((x * sizes[1] + core) * sizes[2] + y, (to[0] * sizes[1] + to[1]) * sizes[2] + to[2])
                )
    return lax.ppermute(array, axes, pairs)


def fit(factors, heads, tails, values):
    shards = lax.axis_size(ENT_BLK)
    ent_dev = factors.shape[0]
    width = heads.shape[3]
    relations = heads.shape[0] * heads.shape[2]
    scale = 1.0 / math.sqrt(shards * width)
    heads = heads.reshape(relations, 1, width)
    tails = tails.reshape(relations, 1, width)
    values = values.reshape(relations, 1, width)
    ents = ent_dev * shards
    table, gram_part, heads, tails, values = tables(factors, heads, tails, values)
    gram = gram_part
    for bit in ("core", "1e", "1o", "2e", "2o"):
        gram = gram + shifted(gram, bit)
    sums = functools.partial(
        triple_sums, heads=heads, tails=tails, values=values, table=table, scale=scale
    )
    upper, lower = {}, {}
    from_partner = {}

    def give(first, after=None):
        partial = sums(first, after=after)
        from_partner[first] = shifted(partial, "core")
        return partial

    def keep(first, after=None):
        upper[first], lower[first] = sums(first, partner=from_partner[first], after=after)

    give(2)
    give(1)
    keep(2)
    third = give(3, upper[2])
    keep(1, third)
    keep(3, upper[1])
    give(0, upper[3])
    keep(0)

    up2 = shifted(upper[2], "1e")
    low2 = shifted(lower[2], "1o")
    up1 = shifted(upper[1], "1e")
    low3 = shifted(lower[3], "1o")
    up_b = shifted(upper[3] + up2, "1o")
    low_b = shifted(lower[1] + low2, "1e")
    up_c = upper[0][1:3] + up1[1:3] + up_b[1:3]
    low_c = lower[0][2:4] + low3[2:4] + low_b[2:4]
    up_c = shifted(up_c, "2e")
    low_c = shifted(low_c, "2o")
    up_d = shifted(upper[0][3] + up1[3] + up_b[3] + up_c[1], "2o")
    low_d = shifted(lower[0][1] + low3[1] + low_b[1] + low_c[0], "2e")
    up_own = upper[0][0] + up1[0] + up_b[0] + up_c[0]
    low_own = lower[0][0] + low3[0] + low_b[0] + low_c[1]

    devices = lax.axis_size(ENT_BLK_REL)
    basis, inner, coef = basis_of(gram, (up_own, up_d, low_own, low_d), devices, ents)
    inner = lax.all_to_all(inner, ENT_BLK_REL, 0, 0, tiled=True)
    return solve(inner, coef, basis)


def solution(mesh):
    torus = Mesh(
        mesh.devices.reshape(mesh.shape["ent"] // 2, 2, mesh.shape["blk"], mesh.shape["rel"]),
        ENT_BLK_REL,
    )
    spread = P(None, "rel", None, ENT_BLK)
    whole = P(ENT_BLK_REL, None, None)
    return jax.shard_map(
        fit,
        mesh=torus,
        in_specs=(P(ENT_BLK, None), spread, spread, spread),
        out_specs=(whole, whole),
        check_vma=False,
    )
```
